768 devices in a mesh: section: 12 (over x, z_hi), dp: 64 (over y, z_lo, core).
Axes of the slice: x: 4, y: 8, z: 12 (z_hi: 3, z_lo: 4; z = z_hi * 4 + z_lo), core: 2. Of those that a mesh axis runs over, the one named last changes fastest.
Arguments:
- buffer: bfloat16 [12, 512, 2048], P('section', 'dp'), may hold values from -6 to 6
- gate_weight: bfloat16 [12, 2, 2048, 8192], P('section', None, None, 'dp'), may hold values from -0.125 to 0.125
- up_weight: bfloat16 [12, 2, 2048, 8192], P('section', None, None, 'dp'), may hold values from -0.125 to 0.125
- down_weight: bfloat16 [12, 2, 8192, 2048], P('section', None, 'dp'), may hold values from -0.09375 to 0.09375
- norm_gain: float32 [12, 2, 2048], P('section'), may hold values from 0.1 to 1.9
- repeat_index: int32 [2, 12], P(None, 'section'), may hold values from 0 to 1
Outputs:
- final_buffer: bfloat16 [12, 512, 2048], P('section', 'dp')
The draws below stay inside these ranges and needn't reach their ends.
Inputs may be any that keep to these rules, and one draw needn't show every extreme that they name: `repeat_index`: the layer each section applies, one of its 2.
All inputs are finite; a program needn't handle non-finite values.
Results may differ from the reference program's by a relative error of at most 0.01.
Values may be sent and summed in bfloat16 or wider, within the bound.
No kernel may reach another device: no remote copies, remote signals or barrier semaphores. Data moves between devices by JAX's collectives and lax.ppermute only.
A program may use at most 32 MiB of HBM per device.

```python
import jax
import jax.numpy as jnp
from jax import lax

D = 2048
FF = 8192
REPEATS = 2
TICKS = 2
SECTIONS = 12
TOKENS = 512


def with_ends(drawn, stream_key, least, largest):
    dims = drawn.shape
    place = [jax.random.randint(jax.random.fold_in(stream_key, axis), (), 0, dims[axis]) for axis in range(len(dims))]
    drawn = drawn.at[tuple(place)].set(least)
    longest = dims.index(max(dims))
    place[longest] = (place[longest] + 1) % dims[longest]
    return drawn.at[tuple(place)].set(largest)


def levels(own_key, extent, split, least, top_value):
    level, own = 1.0, jax.random.fold_in(own_key, 6)
    for axis_at, shards_of in split:
        heights = jnp.exp(jax.random.uniform(jax.random.fold_in(own, axis_at), (shards_of,), jnp.float32, least / len(split), top_value / len(split)))
        level = level * jnp.repeat(heights, extent[axis_at] // shards_of).reshape([-1 if axis == axis_at else 1 for axis in range(len(extent))])
    return level


def noise(stream_key, dims, scale, most, split=(), kind=jnp.bfloat16):
    result = scale * jax.random.normal(stream_key, dims, jnp.float32)
    if split:
        result = result * levels(stream_key, dims, split, -0.22, 0.18)
    return jnp.clip(result, -most, most).astype(kind)


def setup_inputs(seed: int = 0) -> dict:
    key_of = jax.random.split(jax.random.key(seed), 7)
    buffer = noise(key_of[0], (SECTIONS, TOKENS, D), 1.0, 6.0, ((0, 12), (1, 64)))
    gate_weight = noise(key_of[1], (SECTIONS, REPEATS, D, FF), D ** -0.5, 0.125, ((0, 12), (3, 64)))
    up_weight = noise(key_of[2], (SECTIONS, REPEATS, D, FF), D ** -0.5, 0.125, ((0, 12), (3, 64)))
    down_weight = noise(key_of[3], (SECTIONS, REPEATS, FF, D), (FF // 2) ** -0.5, 0.09375, ((0, 12), (2, 64)))
    norm_gain = jnp.clip(1.0 + 0.18 * jax.random.normal(key_of[4], (SECTIONS, REPEATS, D), jnp.float32), 0.1, 1.9)
    repeat_index = with_ends(jax.random.randint(key_of[5], (TICKS, SECTIONS), 0, REPEATS), jax.random.fold_in(key_of[5], 1), 0, REPEATS - 1).astype(jnp.int32)
    return dict(buffer=buffer, gate_weight=gate_weight, up_weight=up_weight, down_weight=down_weight, norm_gain=norm_gain, repeat_index=repeat_index)


epsilon = 0.5

def apply_layer(tokens, gain_row, gate_slab, up_slab, down_slab):
    widened = tokens.astype(jnp.float32)
    squares = lax.optimization_barrier(jnp.mean(widened * widened, axis=-1, keepdims=True))
    normed = (widened * lax.rsqrt(squares + epsilon) * gain_row[None, :]).astype(jnp.bfloat16)
    gate_value = jnp.dot(normed, gate_slab, preferred_element_type=jnp.float32)
    up_value = jnp.dot(normed, up_slab, preferred_element_type=jnp.float32)
    hidden = (jax.nn.silu(gate_value) * up_value).astype(jnp.bfloat16)
    output = jnp.dot(hidden, down_slab, preferred_element_type=jnp.float32)
    return (widened + output).astype(jnp.bfloat16)

def reference(buffer, gate_weight, up_weight, down_weight, norm_gain, repeat_index):
    current = buffer
    for tick_index in range(TICKS):

        def advance(section_index):
            chosen = repeat_index[tick_index, section_index]
            return apply_layer(current[section_index], norm_gain[section_index, chosen], gate_weight[section_index, chosen], up_weight[section_index, chosen], down_weight[section_index, chosen])
        advanced = lax.map(advance, jnp.arange(SECTIONS, dtype=jnp.int32))
        current = jnp.roll(advanced, 1, axis=0)
    return current
```

```python
import jax
import jax.numpy as jnp
from jax import lax
from jax.sharding import PartitionSpec as P

TICKS = 2


epsilon = 0.5


def from_partner(value, axis, bit):
    mask = 2**bit
    pairs = [(source, source ^ mask) for source in range(lax.axis_size(axis))]
    return lax.ppermute(value, axis, pairs)


def passed_along(block, axis, distance):
    devices = range(lax.axis_size(axis))
    route = [((i - distance) % len(devices), i) for i in devices]
    return lax.ppermute(block, axis, route)


def same_core(axis):
    size = lax.axis_size(axis)
    return [[device for device in range(size) if device & 1 == core] for core in range(2)]


def exchange(blocks, axis, groups):
    return lax.all_to_all(blocks, axis, 0, 0, tiled=True, axis_index_groups=groups)


def feed_forward(block_rows, gate_slab, up_slab, down_slab):
    gate_value = jnp.dot(block_rows, gate_slab, preferred_element_type=jnp.float32)
    up_value = jnp.dot(block_rows, up_slab, preferred_element_type=jnp.float32)
    hidden = (jax.nn.silu(gate_value) * up_value).astype(jnp.bfloat16)
    return jnp.dot(hidden, down_slab, preferred_element_type=jnp.float32)


def on_device(buffer, gate_weight, up_weight, down_weight, norm_gain, repeat_index):
    current = buffer[0]
    groups = same_core("dp")
    members = len(groups[0])
    mine = (gate_weight[0], up_weight[0], down_weight[0])
    theirs = from_partner(mine, "dp", 0)
    for tick_index in range(TICKS):
        chosen = repeat_index[tick_index, 0]

        def pick(stack):
            return lax.dynamic_index_in_dim(stack, chosen, 0, keepdims=False)

        gain_row = pick(norm_gain[0])
        gate_both = jnp.concatenate([pick(mine[0]), pick(theirs[0])], axis=1)
        up_both = jnp.concatenate([pick(mine[1]), pick(theirs[1])], axis=1)
        down_both = jnp.concatenate([pick(mine[2]), pick(theirs[2])], axis=0)
        widened = current.astype(jnp.float32)
        squares = jnp.mean(widened * widened, axis=-1, keepdims=True)
        normed = (widened * lax.rsqrt(squares + epsilon) * gain_row[None, :]).astype(jnp.bfloat16)
        rows = normed.shape[0]
        copies = jnp.broadcast_to(normed[None], (members, *normed.shape)).reshape(members * rows, -1)
        group_block = exchange(copies, "dp", groups)
        partial_value = feed_forward(group_block, gate_both, up_both, down_both)
        parts = exchange(partial_value.astype(jnp.bfloat16), "dp", groups)
        output = jnp.sum(parts.reshape(members, rows, -1).astype(jnp.float32), axis=0)
        advanced = (widened + output).astype(jnp.bfloat16)
        current = passed_along(advanced, "section", 1)
    return current[None]


def solution(mesh):
    placed = (
        P("section", "dp", None),
        P("section", None, None, "dp"),
        P("section", None, None, "dp"),
        P("section", None, "dp", None),
        P("section", None, None),
        P(None, "section"),
    )
    return jax.shard_map(
        on_device, mesh=mesh, in_specs=placed, out_specs=P("section", "dp", None), check_vma=False
    )
```

```python
import jax
import jax.numpy as jnp
from jax import lax
from jax.experimental import pallas as pl
from jax.experimental.pallas import tpu as pltpu
from jax.sharding import PartitionSpec as P


TICKS = 2
INTERPRET = False


epsilon = 0.5


def passed_along(block, axis, distance):
    devices = range(lax.axis_size(axis))
    route = [((i - distance) % len(devices), i) for i in devices]
    return lax.ppermute(block, axis, route)


def colour(place):
    return (place >> 1 ^ place >> 3) & 1


def same_kind(axis):
    size = lax.axis_size(axis)
    return [
        [place for place in range(size) if place & 1 == core and colour(place) == shade]
        for core in range(2)
        for shade in range(2)
    ]


def to_other_core(value, axis):
    return lax.ppermute(value, axis, [(place, place ^ 1) for place in range(lax.axis_size(axis))])


def to_other_colour(value, axis):
    size = lax.axis_size(axis)
    route = [(place, place ^ 2 if place & 1 else (place + 8) % size) for place in range(size)]
    return lax.ppermute(value, axis, route)


def exchange(blocks, axis, groups):
    return lax.all_to_all(blocks, axis, 0, 0, tiled=True, axis_index_groups=groups)


def room(mebibytes):
    return pltpu.CompilerParams(vmem_limit_bytes=mebibytes << 20)


def spread_kernel(tick, chosen_ref, rows_ref, gain_ref, copies_ref):
    widened = rows_ref[...].astype(jnp.float32)
    squares = jnp.mean(widened * widened, axis=-1, keepdims=True)
    gain_row = gain_ref[pl.ds(chosen_ref[tick], 1), :]
    normed = (widened * lax.rsqrt(squares + epsilon) * gain_row).astype(copies_ref.dtype)
    for member in range(copies_ref.shape[0]):
        copies_ref[member] = normed


def spread(tick, repeat_index, rows, gains, members):
    count, width = rows.shape
    return pl.pallas_call(
        lambda *refs: spread_kernel(tick, *refs),
        out_shape=jax.ShapeDtypeStruct((members, count, width), rows.dtype),
        in_specs=[
            pl.BlockSpec(memory_space=pltpu.SMEM),
            pl.BlockSpec(memory_space=pltpu.VMEM),
            pl.BlockSpec(memory_space=pltpu.VMEM),
        ],
        out_specs=pl.BlockSpec(memory_space=pltpu.VMEM),
        cost_estimate=pl.CostEstimate(flops=8 * count * width, bytes_accessed=2 * members * count * width, transcendentals=8),
        compiler_params=room(4),
        name="spread",
        interpret=INTERPRET,
    )(repeat_index, rows, gains)


def pack_kernel(chosen_ref, gate_ref, up_ref, down_ref, packed_ref):
    width, lanes = gate_ref.shape[1:]
    packed_ref[0:width] = gate_ref[0]
    packed_ref[width : 2 * width] = up_ref[0]
    for column in range(width // lanes):
        start = 2 * width + column * lanes
        packed_ref[start : start + lanes] = down_ref[0, :, column * lanes : (column + 1) * lanes]


def pack(tick, repeat_index, gate_weight, up_weight, down_weight):
    _, width, lanes = gate_weight.shape
    return pl.pallas_call(
        pack_kernel,
        out_shape=jax.ShapeDtypeStruct((3 * width, lanes), gate_weight.dtype),
        grid_spec=pltpu.PrefetchScalarGridSpec(
            num_scalar_prefetch=1,
            grid=(1,),
            in_specs=[
                pl.BlockSpec((1, width, lanes), lambda _, chosen: (chosen[tick], 0, 0)),
                pl.BlockSpec((1, width, lanes), lambda _, chosen: (chosen[tick], 0, 0)),
                pl.BlockSpec((1, lanes, width), lambda _, chosen: (chosen[tick], 0, 0)),
            ],
            out_specs=pl.BlockSpec((3 * width, lanes), lambda _, chosen: (0, 0)),
        ),
        cost_estimate=pl.CostEstimate(flops=3 * width * lanes, bytes_accessed=12 * width * lanes, transcendentals=0),
        compiler_params=room(8),
        name="pack",
        interpret=INTERPRET,
    )(repeat_index, gate_weight, up_weight, down_weight)


def feed_forward_kernel(tokens_ref, *refs):
    packs, out_ref = refs[:-1], refs[-1]
    members, count, width = tokens_ref.shape
    tokens = tokens_ref[...].reshape(members * count, width)
    lanes = packs[0].shape[1]
    hidden = []
    for packed in packs:
        both = jnp.concatenate([packed[0:width], packed[width : 2 * width]], axis=1)
        value = jnp.dot(tokens, both, preferred_element_type=jnp.float32)
        gate_value, up_value = value[:, :lanes], value[:, lanes:]
        hidden.append((gate_value / (1.0 + jnp.exp(-gate_value)) * up_value).astype(tokens.dtype))
    hidden = jnp.concatenate(hidden, axis=1)
    for column in range(0, width // lanes, 2):
        slabs = []
        for step in range(2):
            start = 2 * width + (column + step) * lanes
            slabs.append(jnp.concatenate([packed[start : start + lanes] for packed in packs], axis=0))
        value = jnp.dot(hidden, jnp.concatenate(slabs, axis=1), preferred_element_type=jnp.float32)
        out_ref[:, :, column * lanes : (column + 2) * lanes] = value.astype(out_ref.dtype).reshape(
            members, count, 2 * lanes
        )


def feed_forward(tokens, packs):
    members, count, width = tokens.shape
    lanes = packs[0].shape[1]
    flops = 6 * members * count * width * lanes * len(packs)
    return pl.pallas_call(
        feed_forward_kernel,
        out_shape=jax.ShapeDtypeStruct(tokens.shape, tokens.dtype),
        in_specs=[pl.BlockSpec(memory_space=pltpu.VMEM)] * (1 + len(packs)),
        out_specs=pl.BlockSpec(memory_space=pltpu.VMEM),
        cost_estimate=pl.CostEstimate(flops=flops, bytes_accessed=6 * width * lanes * len(packs), transcendentals=0),
        compiler_params=room(12),
        name="ffn",
        interpret=INTERPRET,
    )(tokens, *packs)


def advance_kernel(parts_ref, rows_ref, out_ref):
    total = rows_ref[...].astype(jnp.float32)
    output = parts_ref[0].astype(jnp.float32)
    for member in range(1, parts_ref.shape[0]):
        output = output + parts_ref[member].astype(jnp.float32)
    out_ref[...] = (total + output).astype(out_ref.dtype)


def advance(parts, rows):
    return pl.pallas_call(
        advance_kernel,
        out_shape=jax.ShapeDtypeStruct(rows.shape, rows.dtype),
        in_specs=[pl.BlockSpec(memory_space=pltpu.VMEM)] * 2,
        out_specs=pl.BlockSpec(memory_space=pltpu.VMEM),
        cost_estimate=pl.CostEstimate(flops=parts.size, bytes_accessed=2 * parts.size, transcendentals=0),
        compiler_params=room(4),
        name="advance",
        interpret=INTERPRET,
    )(parts, rows)


def on_device(buffer, gate_weight, up_weight, down_weight, norm_gain, repeat_index):
    current = buffer[0]
    chosen = repeat_index.reshape(TICKS)
    groups = same_kind("dp")
    members = len(groups[0])
    for tick in range(TICKS):
        own = pack(tick, chosen, gate_weight[0], up_weight[0], down_weight[0])
        near = to_other_colour(own, "dp")
        own_pair = to_other_core(own, "dp")
        near_pair = to_other_core(near, "dp")
        copies = spread(tick, chosen, current, norm_gain[0], members)
        tokens = exchange(copies, "dp", groups)
        partial_value = feed_forward(tokens, (own, own_pair, near, near_pair))
        parts = exchange(partial_value, "dp", groups)
        advanced = advance(parts, current)
        current = passed_along(advanced, "section", 1)
    return current[None]


def solution(mesh):
    placed = (
        P("section", "dp", None),
        P("section", None, None, "dp"),
        P("section", None, None, "dp"),
        P("section", None, "dp", None),
        P("section", None, None),
        P(None, "section"),
    )
    return jax.shard_map(
        on_device, mesh=mesh, in_specs=placed, out_specs=P("section", "dp", None), check_vma=False
    )
```

```python
import jax
import jax.numpy as jnp
from jax import lax
from jax.experimental import pallas as pl
from jax.experimental.pallas import tpu as pltpu
from jax.sharding import PartitionSpec as P


TICKS = 2
INTERPRET = False


epsilon = 0.5


def passed_along(block, axis, distance):
    devices = range(lax.axis_size(axis))
    route = [((i - distance) % len(devices), i) for i in devices]
    return lax.ppermute(block, axis, route)


def colour(place):
    return (place >> 1 ^ place >> 3) & 1


def same_kind(axis):
    size = lax.axis_size(axis)
    return [
        [place for place in range(size) if place & 1 == core and colour(place) == shade]
        for core in range(2)
        for shade in range(2)
    ]


def to_other_core(value, axis):
    return lax.ppermute(value, axis, [(place, place ^ 1) for place in range(lax.axis_size(axis))])


def to_other_colour(value, axis):
    size = lax.axis_size(axis)
    route = [(place, place ^ 2 if place & 1 else (place + 8) % size) for place in range(size)]
    return lax.ppermute(value, axis, route)


def exchange(blocks, axis, groups):
    return lax.all_to_all(blocks, axis, 0, 0, tiled=True, axis_index_groups=groups)


def room(mebibytes):
    return pltpu.CompilerParams(vmem_limit_bytes=mebibytes << 20)


def spread_kernel(tick, chosen_ref, rows_ref, gain_ref, copies_ref):
    widened = rows_ref[...].astype(jnp.float32)
    squares = jnp.mean(widened * widened, axis=-1, keepdims=True)
    gain_row = gain_ref[pl.ds(chosen_ref[tick], 1), :]
    normed = (widened * lax.rsqrt(squares + epsilon) * gain_row).astype(copies_ref.dtype)
    for member in range(copies_ref.shape[0]):
        copies_ref[member] = normed


def spread(tick, repeat_index, rows, gains, members):
    count, width = rows.shape
    return pl.pallas_call(
        lambda *refs: spread_kernel(tick, *refs),
        out_shape=jax.ShapeDtypeStruct((members, count, width), rows.dtype),
        in_specs=[
            pl.BlockSpec(memory_space=pltpu.SMEM),
            pl.BlockSpec(memory_space=pltpu.VMEM),
            pl.BlockSpec(memory_space=pltpu.VMEM),
        ],
        out_specs=pl.BlockSpec(memory_space=pltpu.VMEM),
        cost_estimate=pl.CostEstimate(flops=8 * count * width, bytes_accessed=2 * members * count * width, transcendentals=8),
        compiler_params=room(4),
        name="spread",
        interpret=INTERPRET,
    )(repeat_index, rows, gains)


def slab_copies(chosen, gate_ref, up_ref, down_ref, packed_ref, arrived):
    width, lanes = gate_ref.shape[1:]
    moves = [
        (gate_ref.at[chosen], packed_ref.at[0:width]),
        (up_ref.at[chosen], packed_ref.at[width : 2 * width]),
    ]
    for column in range(width // lanes):
        start = 2 * width + column * lanes
        moves.append(
            (
                down_ref.at[chosen, :, column * lanes : (column + 1) * lanes],
                packed_ref.at[start : start + lanes],
            )
        )
    return [pltpu.make_async_copy(*move, arrived.at[index]) for index, move in enumerate(moves)]


def pack_kernel(tick, chosen_ref, gate_ref, up_ref, down_ref, packed_ref, arrived):
    copies = slab_copies(chosen_ref[tick], gate_ref, up_ref, down_ref, packed_ref, arrived)
    for copy in copies:
        copy.start()
    for copy in copies:
        copy.wait()


IN_HBM = pl.BlockSpec(memory_space=pltpu.HBM)
IN_VMEM = pl.BlockSpec(memory_space=pltpu.VMEM)
IN_SMEM = pl.BlockSpec(memory_space=pltpu.SMEM)


def pack(tick, chosen, gate_weight, up_weight, down_weight):
    _, width, lanes = gate_weight.shape
    return pl.pallas_call(
        lambda *refs: pack_kernel(tick, *refs),
        out_shape=jax.ShapeDtypeStruct((3 * width, lanes), gate_weight.dtype),
        in_specs=[IN_SMEM, IN_HBM, IN_HBM, IN_HBM],
        out_specs=IN_VMEM,
        scratch_shapes=[pltpu.SemaphoreType.DMA((2 + width // lanes,))],
        cost_estimate=pl.CostEstimate(flops=3 * width * lanes, bytes_accessed=12 * width * lanes, transcendentals=0),
        compiler_params=room(60),
        name="pack",
        interpret=INTERPRET,
    )(chosen, gate_weight, up_weight, down_weight)


def begin_kernel(
    chosen_ref, rows_hbm, gain_hbm, gate_ref, up_ref, down_ref, packed_ref, copies_ref, rows_ref, gain_ref, arrived, loaded
):
    loads = [
        pltpu.make_async_copy(rows_hbm, rows_ref, loaded.at[0]),
        pltpu.make_async_copy(gain_hbm, gain_ref, loaded.at[1]),
    ]
    for load in loads:
        load.start()
    copies = slab_copies(chosen_ref[0], gate_ref, up_ref, down_ref, packed_ref, arrived)
    for copy in copies:
        copy.start()
    for load in loads:
        load.wait()
    spread_kernel(0, chosen_ref, rows_ref, gain_ref, copies_ref)
    for copy in copies:
        copy.wait()


def begin(chosen, rows, gains, gate_weight, up_weight, down_weight, members):
    _, width, lanes = gate_weight.shape
    count = rows.shape[0]
    return pl.pallas_call(
        begin_kernel,
        out_shape=(
            jax.ShapeDtypeStruct((3 * width, lanes), gate_weight.dtype),
            jax.ShapeDtypeStruct((members, count, width), rows.dtype),
        ),
        in_specs=[IN_SMEM] + [IN_HBM] * 5,
        out_specs=(IN_VMEM, IN_VMEM),
        scratch_shapes=[
            pltpu.VMEM(rows.shape, rows.dtype),
            pltpu.VMEM(gains.shape, gains.dtype),
            pltpu.SemaphoreType.DMA((2 + width // lanes,)),
            pltpu.SemaphoreType.DMA((2,)),
        ],
        cost_estimate=pl.CostEstimate(flops=3 * width * lanes, bytes_accessed=12 * width * lanes, transcendentals=8),
        compiler_params=room(60),
        name="begin",
        interpret=INTERPRET,
    )(chosen, rows, gains, gate_weight, up_weight, down_weight)


def feed_forward_kernel(tokens_ref, *refs):
    count = (len(refs) - 2) // 2
    sources, out_ref, packs, arrived = refs[:count], refs[count], refs[count + 1 : -1], refs[-1]
    copies = [
        pltpu.make_async_copy(source, slot, arrived.at[index])
        for index, (source, slot) in enumerate(zip(sources, packs))
    ]
    for copy in copies:
        copy.start()
    members, rows, width = tokens_ref.shape
    tokens = tokens_ref[...].reshape(members * rows, width)
    lanes = packs[0].shape[1]
    hidden = []
    for copy, packed in zip(copies, packs):
        copy.wait()
        both = jnp.concatenate([packed[0:width], packed[width : 2 * width]], axis=1)
        value = jnp.dot(tokens, both, preferred_element_type=jnp.float32)
        gate_value, up_value = value[:, :lanes], value[:, lanes:]
        hidden.append((gate_value / (1.0 + jnp.exp(-gate_value)) * up_value).astype(tokens.dtype))
    hidden = jnp.concatenate(hidden, axis=1)
    for column in range(0, width // lanes, 2):
        slabs = []
        for step in range(2):
            start = 2 * width + (column + step) * lanes
            slabs.append(jnp.concatenate([packed[start : start + lanes] for packed in packs], axis=0))
        value = jnp.dot(hidden, jnp.concatenate(slabs, axis=1), preferred_element_type=jnp.float32)
        out_ref[:, :, column * lanes : (column + 2) * lanes] = value.astype(out_ref.dtype).reshape(
            members, rows, 2 * lanes
        )


def feed_forward(tokens, packs):
    members, rows, width = tokens.shape
    lanes = packs[0].shape[1]
    shards = len(packs)
    return pl.pallas_call(
        feed_forward_kernel,
        out_shape=jax.ShapeDtypeStruct(tokens.shape, tokens.dtype),
        in_specs=[IN_VMEM] + [IN_HBM] * shards,
        out_specs=IN_VMEM,
        scratch_shapes=[pltpu.VMEM(pack.shape, pack.dtype) for pack in packs]
        + [pltpu.SemaphoreType.DMA((shards,))],
        cost_estimate=pl.CostEstimate(
            flops=6 * members * rows * width * lanes * shards,
            bytes_accessed=6 * width * lanes * shards,
            transcendentals=members * rows * lanes * shards,
        ),
        compiler_params=room(62),
        name="ffn",
        interpret=INTERPRET,
    )(tokens, *packs)


def advance_kernel(parts_ref, rows_ref, out_ref):
    total = rows_ref[...].astype(jnp.float32)
    output = parts_ref[0].astype(jnp.float32)
    for member in range(1, parts_ref.shape[0]):
        output = output + parts_ref[member].astype(jnp.float32)
    out_ref[...] = (total + output).astype(out_ref.dtype)


def advance(parts, rows):
    return pl.pallas_call(
        advance_kernel,
        out_shape=jax.ShapeDtypeStruct(rows.shape, rows.dtype),
        in_specs=[pl.BlockSpec(memory_space=pltpu.VMEM)] * 2,
        out_specs=pl.BlockSpec(memory_space=pltpu.VMEM),
        cost_estimate=pl.CostEstimate(flops=parts.size, bytes_accessed=2 * parts.size, transcendentals=0),
        compiler_params=room(4),
        name="advance",
        interpret=INTERPRET,
    )(parts, rows)


def on_device(buffer, gate_weight, up_weight, down_weight, norm_gain, repeat_index):
    current = buffer[0]
    chosen = repeat_index.reshape(TICKS)
    weights = (gate_weight[0], up_weight[0], down_weight[0])
    groups = same_kind("dp")
    members = len(groups[0])
    for tick in range(TICKS):
        if tick == 0:
            own, copies = begin(chosen, current, norm_gain[0], *weights, members)
        else:
            own = pack(tick, chosen, *weights)
            copies = spread(tick, chosen, current, norm_gain[0], members)
        near = to_other_colour(own, "dp")
        tokens = exchange(copies, "dp", groups)
        own_pair = to_other_core(own, "dp")
        near_pair = to_other_core(near, "dp")
        partial_value = feed_forward(tokens, (own, own_pair, near, near_pair))
        parts = exchange(partial_value, "dp", groups)
        advanced = advance(parts, current)
        current = passed_along(advanced, "section", 1)
    return current[None]


def solution(mesh):
    placed = (
        P("section", "dp", None),
        P("section", None, None, "dp"),
        P("section", None, None, "dp"),
        P("section", None, "dp", None),
        P("section", None, None),
        P(None, "section"),
    )
    return jax.shard_map(
        on_device, mesh=mesh, in_specs=placed, out_specs=P("section", "dp", None), check_vma=False
    )
```

```python
import jax
import jax.numpy as jnp
from jax import lax
from jax.experimental import pallas as pl
from jax.experimental.pallas import tpu as pltpu
from jax.sharding import PartitionSpec as P


TICKS = 2
INTERPRET = False


epsilon = 0.5


def passed_along(block, axis, distance):
    devices = range(lax.axis_size(axis))
    route = [((i - distance) % len(devices), i) for i in devices]
    return lax.ppermute(block, axis, route)


def colour(place):
    return (place >> 1 ^ place >> 3) & 1


def same_kind(axis):
    size = lax.axis_size(axis)
    return [
        [place for place in range(size) if place & 1 == core and colour(place) == shade]
        for core in range(2)
        for shade in range(2)
    ]


def to_other_core(value, axis):
    return lax.ppermute(value, axis, [(place, place ^ 1) for place in range(lax.axis_size(axis))])


def to_other_colour(value, axis):
    size = lax.axis_size(axis)
    route = [(place, place ^ 2 if place & 1 else (place + 8) % size) for place in range(size)]
    return lax.ppermute(value, axis, route)


def exchange(blocks, axis, groups):
    return lax.all_to_all(blocks, axis, 0, 0, tiled=True, axis_index_groups=groups)


def room(mebibytes):
    return pltpu.CompilerParams(vmem_limit_bytes=mebibytes << 20)


def spread_kernel(tick, chosen_ref, rows_ref, gain_ref, copies_ref):
    widened = rows_ref[...].astype(jnp.float32)
    squares = jnp.mean(widened * widened, axis=-1, keepdims=True)
    gain_row = gain_ref[pl.ds(chosen_ref[tick], 1), :]
    normed = (widened * lax.rsqrt(squares + epsilon) * gain_row).astype(copies_ref.dtype)
    for member in range(copies_ref.shape[0]):
        copies_ref[member] = normed


def spread(tick, repeat_index, rows, gains, members):
    count, width = rows.shape
    return pl.pallas_call(
        lambda *refs: spread_kernel(tick, *refs),
        out_shape=jax.ShapeDtypeStruct((members, count, width), rows.dtype),
        in_specs=[
            pl.BlockSpec(memory_space=pltpu.SMEM),
            pl.BlockSpec(memory_space=pltpu.VMEM),
            pl.BlockSpec(memory_space=pltpu.VMEM),
        ],
        out_specs=pl.BlockSpec(memory_space=pltpu.VMEM),
        cost_estimate=pl.CostEstimate(flops=8 * count * width, bytes_accessed=2 * members * count * width, transcendentals=8),
        compiler_params=room(4),
        name="spread",
        interpret=INTERPRET,
    )(repeat_index, rows, gains)


def slab_copies(chosen, gate_ref, up_ref, down_ref, packed_ref, arrived):
    width, lanes = gate_ref.shape[1:]
    moves = [
        (gate_ref.at[chosen], packed_ref.at[0:width]),
        (up_ref.at[chosen], packed_ref.at[width : 2 * width]),
    ]
    for column in range(width // lanes):
        start = 2 * width + column * lanes
        moves.append(
            (
                down_ref.at[chosen, :, column * lanes : (column + 1) * lanes],
                packed_ref.at[start : start + lanes],
            )
        )
    return [pltpu.make_async_copy(*move, arrived.at[index]) for index, move in enumerate(moves)]


def pack_kernel(tick, chosen_ref, gate_ref, up_ref, down_ref, packed_ref, arrived):
    copies = slab_copies(chosen_ref[tick], gate_ref, up_ref, down_ref, packed_ref, arrived)
    for copy in copies:
        copy.start()
    for copy in copies:
        copy.wait()


IN_HBM = pl.BlockSpec(memory_space=pltpu.HBM)
IN_VMEM = pl.BlockSpec(memory_space=pltpu.VMEM)
IN_SMEM = pl.BlockSpec(memory_space=pltpu.SMEM)


def pack(tick, chosen, gate_weight, up_weight, down_weight):
    _, width, lanes = gate_weight.shape
    return pl.pallas_call(
        lambda *refs: pack_kernel(tick, *refs),
        out_shape=jax.ShapeDtypeStruct((3 * width, lanes), gate_weight.dtype),
        in_specs=[IN_SMEM, IN_HBM, IN_HBM, IN_HBM],
        out_specs=IN_VMEM,
        scratch_shapes=[pltpu.SemaphoreType.DMA((2 + width // lanes,))],
        cost_estimate=pl.CostEstimate(flops=3 * width * lanes, bytes_accessed=12 * width * lanes, transcendentals=0),
        compiler_params=room(60),
        name="pack",
        interpret=INTERPRET,
    )(chosen, gate_weight, up_weight, down_weight)


def begin_kernel(
    chosen_ref, rows_hbm, gain_hbm, gate_ref, up_ref, down_ref, packed_ref, copies_ref, rows_ref, gain_ref, arrived, loaded
):
    loads = [
        pltpu.make_async_copy(rows_hbm, rows_ref, loaded.at[0]),
        pltpu.make_async_copy(gain_hbm, gain_ref, loaded.at[1]),
    ]
    for load in loads:
        load.start()
    copies = slab_copies(chosen_ref[0], gate_ref, up_ref, down_ref, packed_ref, arrived)
    for copy in copies:
        copy.start()
    for load in loads:
        load.wait()
    spread_kernel(0, chosen_ref, rows_ref, gain_ref, copies_ref)
    for copy in copies:
        copy.wait()


def begin(chosen, rows, gains, gate_weight, up_weight, down_weight, members):
    _, width, lanes = gate_weight.shape
    count = rows.shape[0]
    return pl.pallas_call(
        begin_kernel,
        out_shape=(
            jax.ShapeDtypeStruct((3 * width, lanes), gate_weight.dtype),
            jax.ShapeDtypeStruct((members, count, width), rows.dtype),
        ),
        in_specs=[IN_SMEM] + [IN_HBM] * 5,
        out_specs=(IN_VMEM, IN_VMEM),
        scratch_shapes=[
            pltpu.VMEM(rows.shape, rows.dtype),
            pltpu.VMEM(gains.shape, gains.dtype),
            pltpu.SemaphoreType.DMA((2 + width // lanes,)),
            pltpu.SemaphoreType.DMA((2,)),
        ],
        cost_estimate=pl.CostEstimate(flops=3 * width * lanes, bytes_accessed=12 * width * lanes, transcendentals=8),
        compiler_params=room(60),
        name="begin",
        interpret=INTERPRET,
    )(chosen, rows, gains, gate_weight, up_weight, down_weight)


def feed_forward_kernel(tokens_ref, own_ref, *refs):
    count = (len(refs) - 2) // 2
    sources, out_ref, held, arrived = refs[:count], refs[count], refs[count + 1 : -1], refs[-1]
    members, rows, width = tokens_ref.shape
    parts = ((0, 2 * width), (2 * width, 3 * width))
    copies = [
        [
            pltpu.make_async_copy(source.at[start:end], slot.at[start:end], arrived.at[part, index])
            for index, (source, slot) in enumerate(zip(sources, held))
        ]
        for part, (start, end) in enumerate(parts)
    ]
    for part in copies:
        for copy in part:
            copy.start()
    tokens = tokens_ref[...].reshape(members * rows, width)
    packs = (own_ref, *held)
    lanes = own_ref.shape[1]
    hidden = []
    for index, packed in enumerate(packs):
        if index:
            copies[0][index - 1].wait()
        both = jnp.concatenate([packed[0:width], packed[width : 2 * width]], axis=1)
        value = jnp.dot(tokens, both, preferred_element_type=jnp.float32)
        gate_value, up_value = value[:, :lanes], value[:, lanes:]
        hidden.append((gate_value / (1.0 + jnp.exp(-gate_value)) * up_value).astype(tokens.dtype))
    hidden = jnp.concatenate(hidden, axis=1)
    for copy in copies[1]:
        copy.wait()
    for column in range(0, width // lanes, 2):
        slabs = []
        for step in range(2):
            start = 2 * width + (column + step) * lanes
            slabs.append(jnp.concatenate([packed[start : start + lanes] for packed in packs], axis=0))
        value = jnp.dot(hidden, jnp.concatenate(slabs, axis=1), preferred_element_type=jnp.float32)
        out_ref[:, :, column * lanes : (column + 2) * lanes] = value.astype(out_ref.dtype).reshape(
            members, rows, 2 * lanes
        )


def feed_forward(tokens, own, others):
    members, rows, width = tokens.shape
    lanes = own.shape[1]
    shards = 1 + len(others)
    return pl.pallas_call(
        feed_forward_kernel,
        out_shape=jax.ShapeDtypeStruct(tokens.shape, tokens.dtype),
        in_specs=[IN_VMEM, IN_VMEM] + [IN_HBM] * len(others),
        out_specs=IN_VMEM,
        scratch_shapes=[pltpu.VMEM(own.shape, own.dtype) for _ in others]
        + [pltpu.SemaphoreType.DMA((2, len(others)))],
        cost_estimate=pl.CostEstimate(
            flops=6 * members * rows * width * lanes * shards,
            bytes_accessed=6 * width * lanes * shards,
            transcendentals=members * rows * lanes * shards,
        ),
        compiler_params=room(8),
        name="ffn",
        interpret=INTERPRET,
    )(tokens, own, *others)


def advance_kernel(parts_ref, rows_ref, out_ref):
    total = rows_ref[...].astype(jnp.float32)
    output = parts_ref[0].astype(jnp.float32)
    for member in range(1, parts_ref.shape[0]):
        output = output + parts_ref[member].astype(jnp.float32)
    out_ref[...] = (total + output).astype(out_ref.dtype)


def advance(parts, rows):
    return pl.pallas_call(
        advance_kernel,
        out_shape=jax.ShapeDtypeStruct(rows.shape, rows.dtype),
        in_specs=[pl.BlockSpec(memory_space=pltpu.VMEM)] * 2,
        out_specs=pl.BlockSpec(memory_space=pltpu.VMEM),
        cost_estimate=pl.CostEstimate(flops=parts.size, bytes_accessed=2 * parts.size, transcendentals=0),
        compiler_params=room(4),
        name="advance",
        interpret=INTERPRET,
    )(parts, rows)


def on_device(buffer, gate_weight, up_weight, down_weight, norm_gain, repeat_index):
    current = buffer[0]
    chosen = repeat_index.reshape(TICKS)
    weights = (gate_weight[0], up_weight[0], down_weight[0])
    groups = same_kind("dp")
    members = len(groups[0])
    for tick in range(TICKS):
        if tick == 0:
            own, copies = begin(chosen, current, norm_gain[0], *weights, members)
        else:
            own = pack(tick, chosen, *weights)
            copies = spread(tick, chosen, current, norm_gain[0], members)
        near = to_other_colour(own, "dp")
        tokens = exchange(copies, "dp", groups)
        own_pair = to_other_core(own, "dp")
        near_pair = to_other_core(near, "dp")
        partial_value = feed_forward(tokens, own, (own_pair, near, near_pair))
        parts = exchange(partial_value, "dp", groups)
        advanced = advance(parts, current)
        current = passed_along(advanced, "section", 1)
    return current[None]


def solution(mesh):
    placed = (
        P("section", "dp", None),
        P("section", None, None, "dp"),
        P("section", None, None, "dp"),
        P("section", None, "dp", None),
        P("section", None, None),
        P(None, "section"),
    )
    return jax.shard_map(
        on_device, mesh=mesh, in_specs=placed, out_specs=P("section", "dp", None), check_vma=False
    )
```

```python
import jax
import jax.numpy as jnp
from jax import lax
from jax.experimental import pallas as pl
from jax.experimental.pallas import tpu as pltpu
from jax.sharding import PartitionSpec as P


TICKS = 2
INTERPRET = False


epsilon = 0.5


def passed_along(block, axis, distance):
    devices = range(lax.axis_size(axis))
    route = [((i - distance) % len(devices), i) for i in devices]
    return lax.ppermute(block, axis, route)


def colour(place):
    return (place >> 1 ^ place >> 3) & 1


def same_kind(axis):
    size = lax.axis_size(axis)
    return [
        [place for place in range(size) if place & 1 == core and colour(place) == shade]
        for core in range(2)
        for shade in range(2)
    ]


def to_other_core(value, axis):
    return lax.ppermute(value, axis, [(place, place ^ 1) for place in range(lax.axis_size(axis))])


def to_other_colour(value, axis, step):
    size = lax.axis_size(axis)
    route = [(place, place ^ 2 if place & 1 else (place + 8 * step) % size) for place in range(size)]
    return lax.ppermute(value, axis, route)


def exchange(blocks, axis, groups):
    return lax.all_to_all(blocks, axis, 0, 0, tiled=True, axis_index_groups=groups)


def room(mebibytes):
    return pltpu.CompilerParams(vmem_limit_bytes=mebibytes << 20)


def spread_kernel(tick, chosen_ref, rows_ref, gain_ref, copies_ref):
    widened = rows_ref[...].astype(jnp.float32)
    squares = jnp.mean(widened * widened, axis=-1, keepdims=True)
    gain_row = gain_ref[pl.ds(chosen_ref[tick], 1), :]
    normed = (widened * lax.rsqrt(squares + epsilon) * gain_row).astype(copies_ref.dtype)
    for member in range(copies_ref.shape[0]):
        copies_ref[member] = normed


def spread(tick, repeat_index, rows, gains, members):
    count, width = rows.shape
    return pl.pallas_call(
        lambda *refs: spread_kernel(tick, *refs),
        out_shape=jax.ShapeDtypeStruct((members, count, width), rows.dtype),
        in_specs=[
            pl.BlockSpec(memory_space=pltpu.SMEM),
            pl.BlockSpec(memory_space=pltpu.VMEM),
            pl.BlockSpec(memory_space=pltpu.VMEM),
        ],
        out_specs=pl.BlockSpec(memory_space=pltpu.VMEM),
        cost_estimate=pl.CostEstimate(flops=8 * count * width, bytes_accessed=2 * members * count * width, transcendentals=8),
        compiler_params=room(4),
        name="spread",
        interpret=INTERPRET,
    )(repeat_index, rows, gains)


def slab_copies(chosen, gate_ref, up_ref, down_ref, packed_ref, arrived):
    width, lanes = gate_ref.shape[1:]
    moves = [
        (gate_ref.at[chosen], packed_ref.at[0:width]),
        (up_ref.at[chosen], packed_ref.at[width : 2 * width]),
    ]
    for column in range(width // lanes):
        start = 2 * width + column * lanes
        moves.append(
            (
                down_ref.at[chosen, :, column * lanes : (column + 1) * lanes],
                packed_ref.at[start : start + lanes],
            )
        )
    return [pltpu.make_async_copy(*move, arrived.at[index]) for index, move in enumerate(moves)]


def pack_kernel(tick, chosen_ref, gate_ref, up_ref, down_ref, packed_ref, arrived):
    copies = slab_copies(chosen_ref[tick], gate_ref, up_ref, down_ref, packed_ref, arrived)
    for copy in copies:
        copy.start()
    for copy in copies:
        copy.wait()


IN_HBM = pl.BlockSpec(memory_space=pltpu.HBM)
IN_VMEM = pl.BlockSpec(memory_space=pltpu.VMEM)
IN_SMEM = pl.BlockSpec(memory_space=pltpu.SMEM)


def pack(tick, chosen, gate_weight, up_weight, down_weight):
    _, width, lanes = gate_weight.shape
    return pl.pallas_call(
        lambda *refs: pack_kernel(tick, *refs),
        out_shape=jax.ShapeDtypeStruct((3 * width, lanes), gate_weight.dtype),
        in_specs=[IN_SMEM, IN_HBM, IN_HBM, IN_HBM],
        out_specs=IN_VMEM,
        scratch_shapes=[pltpu.SemaphoreType.DMA((2 + width // lanes,))],
        cost_estimate=pl.CostEstimate(flops=3 * width * lanes, bytes_accessed=12 * width * lanes, transcendentals=0),
        compiler_params=room(60),
        name="pack",
        interpret=INTERPRET,
    )(chosen, gate_weight, up_weight, down_weight)


def begin_kernel(
    chosen_ref, rows_hbm, gain_hbm, gate_ref, up_ref, down_ref, packed_ref, copies_ref, rows_ref, gain_ref, arrived, loaded
):
    loads = [
        pltpu.make_async_copy(rows_hbm, rows_ref, loaded.at[0]),
        pltpu.make_async_copy(gain_hbm, gain_ref, loaded.at[1]),
    ]
    for load in loads:
        load.start()
    copies = slab_copies(chosen_ref[0], gate_ref, up_ref, down_ref, packed_ref, arrived)
    for copy in copies:
        copy.start()
    for load in loads:
        load.wait()
    spread_kernel(0, chosen_ref, rows_ref, gain_ref, copies_ref)
    for copy in copies:
        copy.wait()


def begin(chosen, rows, gains, gate_weight, up_weight, down_weight, members):
    _, width, lanes = gate_weight.shape
    count = rows.shape[0]
    return pl.pallas_call(
        begin_kernel,
        out_shape=(
            jax.ShapeDtypeStruct((3 * width, lanes), gate_weight.dtype),
            jax.ShapeDtypeStruct((members, count, width), rows.dtype),
        ),
        in_specs=[IN_SMEM] + [IN_HBM] * 5,
        out_specs=(IN_VMEM, IN_VMEM),
        scratch_shapes=[
            pltpu.VMEM(rows.shape, rows.dtype),
            pltpu.VMEM(gains.shape, gains.dtype),
            pltpu.SemaphoreType.DMA((2 + width // lanes,)),
            pltpu.SemaphoreType.DMA((2,)),
        ],
        cost_estimate=pl.CostEstimate(flops=3 * width * lanes, bytes_accessed=12 * width * lanes, transcendentals=8),
        compiler_params=room(60),
        name="begin",
        interpret=INTERPRET,
    )(chosen, rows, gains, gate_weight, up_weight, down_weight)


def feed_forward_kernel(tokens_ref, own_ref, *refs):
    count = (len(refs) - 2) // 2
    sources, out_ref, held, arrived = refs[:count], refs[count], refs[count + 1 : -1], refs[-1]
    members, rows, width = tokens_ref.shape
    parts = ((0, 2 * width), (2 * width, 3 * width))
    copies = [
        [
            pltpu.make_async_copy(source.at[start:end], slot.at[start:end], arrived.at[part, index])
            for index, (source, slot) in enumerate(zip(sources, held))
        ]
        for part, (start, end) in enumerate(parts)
    ]
    for part in copies:
        for copy in part:
            copy.start()
    tokens = tokens_ref[...].reshape(members * rows, width)
    packs = (own_ref, *held)
    lanes = own_ref.shape[1]
    hidden = []
    for index, packed in enumerate(packs):
        if index:
            copies[0][index - 1].wait()
        both = jnp.concatenate([packed[0:width], packed[width : 2 * width]], axis=1)
        value = jnp.dot(tokens, both, preferred_element_type=jnp.float32)
        gate_value, up_value = value[:, :lanes], value[:, lanes:]
        hidden.append((gate_value / (1.0 + jnp.exp(-gate_value)) * up_value).astype(tokens.dtype))
    hidden = jnp.concatenate(hidden, axis=1)
    for copy in copies[1]:
        copy.wait()
    for column in range(0, width // lanes, 2):
        slabs = []
        for step in range(2):
            start = 2 * width + (column + step) * lanes
            slabs.append(jnp.concatenate([packed[start : start + lanes] for packed in packs], axis=0))
        value = jnp.dot(hidden, jnp.concatenate(slabs, axis=1), preferred_element_type=jnp.float32)
        out_ref[:, :, column * lanes : (column + 2) * lanes] = value.astype(out_ref.dtype).reshape(
            members, rows, 2 * lanes
        )


def feed_forward(tokens, own, others):
    members, rows, width = tokens.shape
    lanes = own.shape[1]
    shards = 1 + len(others)
    return pl.pallas_call(
        feed_forward_kernel,
        out_shape=jax.ShapeDtypeStruct(tokens.shape, tokens.dtype),
        in_specs=[IN_VMEM, IN_VMEM] + [IN_HBM] * len(others),
        out_specs=IN_VMEM,
        scratch_shapes=[pltpu.VMEM(own.shape, own.dtype) for _ in others]
        + [pltpu.SemaphoreType.DMA((2, len(others)))],
        cost_estimate=pl.CostEstimate(
            flops=6 * members * rows * width * lanes * shards,
            bytes_accessed=6 * width * lanes * shards,
            transcendentals=members * rows * lanes * shards,
        ),
        compiler_params=room(8),
        name="ffn",
        interpret=INTERPRET,
    )(tokens, own, *others)


def advance_kernel(parts_ref, rows_ref, out_ref):
    total = rows_ref[...].astype(jnp.float32)
    output = parts_ref[0].astype(jnp.float32)
    for member in range(1, parts_ref.shape[0]):
        output = output + parts_ref[member].astype(jnp.float32)
    out_ref[...] = (total + output).astype(out_ref.dtype)


def advance(parts, rows):
    return pl.pallas_call(
        advance_kernel,
        out_shape=jax.ShapeDtypeStruct(rows.shape, rows.dtype),
        in_specs=[pl.BlockSpec(memory_space=pltpu.VMEM)] * 2,
        out_specs=pl.BlockSpec(memory_space=pltpu.VMEM),
        cost_estimate=pl.CostEstimate(flops=parts.size, bytes_accessed=2 * parts.size, transcendentals=0),
        compiler_params=room(4),
        name="advance",
        interpret=INTERPRET,
    )(parts, rows)


def on_device(buffer, gate_weight, up_weight, down_weight, norm_gain, repeat_index):
    current = buffer[0]
    chosen = repeat_index.reshape(TICKS)
    weights = (gate_weight[0], up_weight[0], down_weight[0])
    groups = same_kind("dp")
    members = len(groups[0])
    for tick in range(TICKS):
        if tick == 0:
            own, copies = begin(chosen, current, norm_gain[0], *weights, members)
        else:
            own = pack(tick, chosen, *weights)
            copies = spread(tick, chosen, current, norm_gain[0], members)
        near = to_other_colour(own, "dp", 1 if tick else -1)
        tokens = exchange(copies, "dp", groups)
        own_pair = to_other_core(own, "dp")
        near_pair = to_other_core(near, "dp")
        partial_value = feed_forward(tokens, own, (own_pair, near, near_pair))
        parts = exchange(partial_value, "dp", groups)
        advanced = advance(parts, current)
        current = passed_along(advanced, "section", 1)
    return current[None]


def solution(mesh):
    placed = (
        P("section", "dp", None),
        P("section", None, None, "dp"),
        P("section", None, None, "dp"),
        P("section", None, "dp", None),
        P("section", None, None),
        P(None, "section"),
    )
    return jax.shard_map(
        on_device, mesh=mesh, in_specs=placed, out_specs=P("section", "dp", None), check_vma=False
    )
```

```python
import jax
import jax.numpy as jnp
from jax import lax
from jax.experimental import pallas as pl
from jax.experimental.pallas import tpu as pltpu
from jax.sharding import PartitionSpec as P


TICKS = 2
INTERPRET = False


epsilon = 0.5


def passed_along(block, axis, distance):
    devices = range(lax.axis_size(axis))
    route = [((i - distance) % len(devices), i) for i in devices]
    return lax.ppermute(block, axis, route)


def colour(place):
    return (place >> 1 ^ place >> 3) & 1


def same_kind(axis):
    size = lax.axis_size(axis)
    return [
        [place for place in range(size) if place & 1 == core and colour(place) == shade]
        for core in range(2)
        for shade in range(2)
    ]


def to_other_core(value, axis):
    return lax.ppermute(value, axis, [(place, place ^ 1) for place in range(lax.axis_size(axis))])


def to_other_colour(value, axis, step):
    size = lax.axis_size(axis)
    route = [(place, place ^ 2 if place & 1 else (place + 8 * step) % size) for place in range(size)]
    return lax.ppermute(value, axis, route)


def exchange(blocks, axis, groups):
    return lax.all_to_all(blocks, axis, 0, 0, tiled=True, axis_index_groups=groups)


def room(mebibytes):
    return pltpu.CompilerParams(vmem_limit_bytes=mebibytes << 20)


def spread_kernel(tick, chosen_ref, rows_ref, gain_ref, copies_ref):
    widened = rows_ref[...].astype(jnp.float32)
    squares = jnp.mean(widened * widened, axis=-1, keepdims=True)
    gain_row = gain_ref[pl.ds(chosen_ref[tick], 1), :]
    normed = (widened * lax.rsqrt(squares + epsilon) * gain_row).astype(copies_ref.dtype)
    for member in range(copies_ref.shape[0]):
        copies_ref[member] = normed


def spread(tick, repeat_index, rows, gains, members):
    count, width = rows.shape
    return pl.pallas_call(
        lambda *refs: spread_kernel(tick, *refs),
        out_shape=jax.ShapeDtypeStruct((members, count, width), rows.dtype),
        in_specs=[
            pl.BlockSpec(memory_space=pltpu.SMEM),
            pl.BlockSpec(memory_space=pltpu.VMEM),
            pl.BlockSpec(memory_space=pltpu.VMEM),
        ],
        out_specs=pl.BlockSpec(memory_space=pltpu.VMEM),
        cost_estimate=pl.CostEstimate(flops=8 * count * width, bytes_accessed=2 * members * count * width, transcendentals=8),
        compiler_params=room(4),
        name="spread",
        interpret=INTERPRET,
    )(repeat_index, rows, gains)


def slab_loads(chosen, sources, slabs, arrived):
    return [
        pltpu.make_async_copy(source.at[chosen], slab, arrived.at[index])
        for index, (source, slab) in enumerate(zip(sources, slabs))
    ]


def store_halves(gate_ref, up_ref, down_ref, half_refs):
    width, lanes = gate_ref.shape
    units = lanes // 2
    gate_value = gate_ref[...].astype(jnp.float32)
    up_value = up_ref[...].astype(jnp.float32)
    first = lax.broadcasted_iota(jnp.int32, (width, lanes), 1) < units
    mixed = (
        jnp.where(first, gate_value, pltpu.roll(up_value, units, 1)),
        jnp.where(first, pltpu.roll(gate_value, units, 1), up_value),
    )
    for half, half_ref in enumerate(half_refs):
        half_ref[0:width] = mixed[half].astype(half_ref.dtype)
        for column in range(width // lanes):
            start = width + column * units
            half_ref[start : start + units] = down_ref[
                half * units : (half + 1) * units, column * lanes : (column + 1) * lanes
            ]


def pack_kernel(tick, chosen_ref, gate_hbm, up_hbm, down_hbm, packed_ref, *scratch):
    slabs, arrived = scratch[:-1], scratch[-1]
    loads = slab_loads(chosen_ref[tick], (gate_hbm, up_hbm, down_hbm), slabs, arrived)
    for load in loads:
        load.start()
    for load in loads:
        load.wait()
    store_halves(*slabs, halves_in(packed_ref, slabs[0].shape[0]))


def halves_in(ref, width):
    size = width + width // 2
    return [ref.at[start : start + size] for start in range(0, ref.shape[0], size)]


IN_HBM = pl.BlockSpec(memory_space=pltpu.HBM)
IN_VMEM = pl.BlockSpec(memory_space=pltpu.VMEM)
IN_SMEM = pl.BlockSpec(memory_space=pltpu.SMEM)


def halves_of(weight):
    _, width, lanes = weight.shape
    half = jax.ShapeDtypeStruct((width + width // 2, lanes), weight.dtype)
    return half, half


def slabs_of(*weights):
    return [pltpu.VMEM(weight.shape[1:], weight.dtype) for weight in weights]


def pack(tick, chosen, *weights):
    size = weights[0].shape[1] * weights[0].shape[2]
    return pl.pallas_call(
        lambda *refs: pack_kernel(tick, *refs),
        out_shape=jax.ShapeDtypeStruct((3 * weights[0].shape[1], weights[0].shape[2]), weights[0].dtype),
        in_specs=[IN_SMEM, IN_HBM, IN_HBM, IN_HBM],
        out_specs=IN_VMEM,
        scratch_shapes=slabs_of(*weights) + [pltpu.SemaphoreType.DMA((3,))],
        cost_estimate=pl.CostEstimate(flops=6 * size, bytes_accessed=12 * size, transcendentals=0),
        compiler_params=room(60),
        name="pack",
        interpret=INTERPRET,
    )(chosen, *weights)


def begin_kernel(
    chosen_ref, rows_hbm, gain_hbm, gate_hbm, up_hbm, down_hbm, first_ref, second_ref, copies_ref, *scratch
):
    slabs, (rows_ref, gain_ref, arrived, loaded) = scratch[:3], scratch[3:]
    early = [
        pltpu.make_async_copy(rows_hbm, rows_ref, loaded.at[0]),
        pltpu.make_async_copy(gain_hbm, gain_ref, loaded.at[1]),
    ]
    for load in early:
        load.start()
    loads = slab_loads(chosen_ref[0], (gate_hbm, up_hbm, down_hbm), slabs, arrived)
    for load in loads:
        load.start()
    for load in early:
        load.wait()
    spread_kernel(0, chosen_ref, rows_ref, gain_ref, copies_ref)
    for load in loads:
        load.wait()
    store_halves(*slabs, (first_ref, second_ref))


def begin(chosen, rows, gains, weights, members):
    size = weights[0].shape[1] * weights[0].shape[2]
    return pl.pallas_call(
        begin_kernel,
        out_shape=(*halves_of(weights[0]), jax.ShapeDtypeStruct((members, *rows.shape), rows.dtype)),
        in_specs=[IN_SMEM] + [IN_HBM] * 5,
        out_specs=(IN_VMEM,) * 3,
        scratch_shapes=slabs_of(*weights)
        + [
            pltpu.VMEM(rows.shape, rows.dtype),
            pltpu.VMEM(gains.shape, gains.dtype),
            pltpu.SemaphoreType.DMA((3,)),
            pltpu.SemaphoreType.DMA((2,)),
        ],
        cost_estimate=pl.CostEstimate(flops=6 * size, bytes_accessed=12 * size, transcendentals=8),
        compiler_params=room(60),
        name="begin",
        interpret=INTERPRET,
    )(chosen, rows, gains, *weights)


def feed_forward_kernel(owned, tokens_ref, *refs):
    own, refs = refs[:owned], refs[owned:]
    count = (len(refs) - 2) // 2
    sources, out_ref, held, arrived = refs[:count], refs[count], refs[count + 1 : -1], refs[-1]
    members, rows, width = tokens_ref.shape

    def split(refs):
        return [half for ref in refs for half in halves_in(ref, width)]

    parts = ((0, width), (width, width + width // 2))
    copies = [
        [
            pltpu.make_async_copy(source.at[start:end], slot.at[start:end], arrived.at[part, index])
            for index, (source, slot) in enumerate(zip(split(sources), split(held)))
        ]
        for part, (start, end) in enumerate(parts)
    ]
    for part in copies:
        for copy in part:
            copy.start()
    tokens = tokens_ref[...].reshape(members * rows, width)
    halves = split(own) + split(held)
    lanes = own[0].shape[1]
    units = lanes // 2
    first = lax.broadcasted_iota(jnp.int32, (members * rows, lanes), 1) < units
    hidden = []
    for index in range(0, len(halves), 2):
        if index:
            copies[0][index - 2].wait()
            copies[0][index - 1].wait()
        both = jnp.concatenate([halves[index][0:width], halves[index + 1][0:width]], axis=1)
        value = jnp.dot(tokens, both, preferred_element_type=jnp.float32)
        left, right = value[:, :lanes], value[:, lanes:]
        gate_value = jnp.where(first, left, pltpu.roll(right, units, 1))
        up_value = jnp.where(first, pltpu.roll(left, units, 1), right)
        hidden.append((gate_value / (1.0 + jnp.exp(-gate_value)) * up_value).astype(tokens.dtype))
    hidden = jnp.concatenate(hidden, axis=1)
    for copy in copies[1]:
        copy.wait()
    for column in range(0, width // lanes, 2):
        slabs = []
        for step in range(2):
            start = width + (column + step) * units
            slabs.append(jnp.concatenate([half[start : start + units] for half in halves], axis=0))
        value = jnp.dot(hidden, jnp.concatenate(slabs, axis=1), preferred_element_type=jnp.float32)
        out_ref[:, :, column * lanes : (column + 2) * lanes] = value.astype(out_ref.dtype).reshape(
            members, rows, 2 * lanes
        )


def feed_forward(tokens, own, others):
    members, rows, width = tokens.shape
    lanes = own[0].shape[1]
    halves = 8
    return pl.pallas_call(
        lambda *refs: feed_forward_kernel(len(own), *refs),
        out_shape=jax.ShapeDtypeStruct(tokens.shape, tokens.dtype),
        in_specs=[IN_VMEM] * (1 + len(own)) + [IN_HBM] * len(others),
        out_specs=IN_VMEM,
        scratch_shapes=[pltpu.VMEM(other.shape, other.dtype) for other in others]
        + [pltpu.SemaphoreType.DMA((2, halves - 2))],
        cost_estimate=pl.CostEstimate(
            flops=3 * members * rows * width * lanes * halves,
            bytes_accessed=3 * width * lanes * halves,
            transcendentals=members * rows * lanes * halves // 2,
        ),
        compiler_params=room(8),
        name="ffn",
        interpret=INTERPRET,
    )(tokens, *own, *others)


def advance_kernel(parts_ref, rows_ref, out_ref):
    total = rows_ref[...].astype(jnp.float32)
    output = parts_ref[0].astype(jnp.float32)
    for member in range(1, parts_ref.shape[0]):
        output = output + parts_ref[member].astype(jnp.float32)
    out_ref[...] = (total + output).astype(out_ref.dtype)


def advance(parts, rows):
    return pl.pallas_call(
        advance_kernel,
        out_shape=jax.ShapeDtypeStruct(rows.shape, rows.dtype),
        in_specs=[pl.BlockSpec(memory_space=pltpu.VMEM)] * 2,
        out_specs=pl.BlockSpec(memory_space=pltpu.VMEM),
        cost_estimate=pl.CostEstimate(flops=parts.size, bytes_accessed=2 * parts.size, transcendentals=0),
        compiler_params=room(4),
        name="advance",
        interpret=INTERPRET,
    )(parts, rows)


def on_device(buffer, gate_weight, up_weight, down_weight, norm_gain, repeat_index):
    current = buffer[0]
    chosen = repeat_index.reshape(TICKS)
    weights = (gate_weight[0], up_weight[0], down_weight[0])
    groups = same_kind("dp")
    members = len(groups[0])
    for tick in range(TICKS):
        if tick == 0:
            *own, copies = begin(chosen, current, norm_gain[0], weights, members)
        else:
            own = [pack(tick, chosen, *weights)]
            copies = spread(tick, chosen, current, norm_gain[0], members)
        near, pair, far = [], [], []
        for index, packed in enumerate(own):
            near.append(to_other_colour(packed, "dp", 1 if tick or index else -1))
            pair.append(to_other_core(packed, "dp"))
            far.append(to_other_core(near[-1], "dp"))
        tokens = exchange(copies, "dp", groups)
        partial_value = feed_forward(tokens, own, (*pair, *near, *far))
        parts = exchange(partial_value, "dp", groups)
        advanced = advance(parts, current)
        current = passed_along(advanced, "section", 1)
    return current[None]


def solution(mesh):
    placed = (
        P("section", "dp", None),
        P("section", None, None, "dp"),
        P("section", None, None, "dp"),
        P("section", None, "dp", None),
        P("section", None, None),
        P(None, "section"),
    )
    return jax.shard_map(
        on_device, mesh=mesh, in_specs=placed, out_specs=P("section", "dp", None), check_vma=False
    )
```

```python
import jax
import jax.numpy as jnp
from jax import lax
from jax.experimental import pallas as pl
from jax.experimental.pallas import tpu as pltpu
from jax.sharding import PartitionSpec as P


TICKS = 2
INTERPRET = False


epsilon = 0.5


def passed_along(block, axis, distance):
    devices = range(lax.axis_size(axis))
    route = [((i - distance) % len(devices), i) for i in devices]
    return lax.ppermute(block, axis, route)


def colour(place):
    return (place >> 1 ^ place >> 3) & 1


def same_kind(axis):
    places = sorted(range(lax.axis_size(axis)), key=lambda place: (place & 7, place))
    return [
        [place for place in places if place & 1 == core and colour(place) == shade]
        for core in range(2)
        for shade in range(2)
    ]


def to_other_core(value, axis):
    return lax.ppermute(value, axis, [(place, place ^ 1) for place in range(lax.axis_size(axis))])


def to_other_colour(value, axis, step):
    size = lax.axis_size(axis)
    route = [(place, place ^ 2 if place & 1 else (place + 8 * step) % size) for place in range(size)]
    return lax.ppermute(value, axis, route)


def exchange(blocks, axis, groups):
    return lax.all_to_all(blocks, axis, 0, 0, tiled=True, axis_index_groups=groups)


def room(mebibytes):
    return pltpu.CompilerParams(vmem_limit_bytes=mebibytes << 20)


def spread_kernel(tick, chosen_ref, rows_ref, gain_ref, copies_ref):
    widened = rows_ref[...].astype(jnp.float32)
    squares = jnp.mean(widened * widened, axis=-1, keepdims=True)
    gain_row = gain_ref[pl.ds(chosen_ref[tick], 1), :]
    normed = (widened * lax.rsqrt(squares + epsilon) * gain_row).astype(copies_ref.dtype)
    for member in range(copies_ref.shape[0]):
        copies_ref[member] = normed


def spread(tick, repeat_index, rows, gains, members):
    count, width = rows.shape
    return pl.pallas_call(
        lambda *refs: spread_kernel(tick, *refs),
        out_shape=jax.ShapeDtypeStruct((members, count, width), rows.dtype),
        in_specs=[
            pl.BlockSpec(memory_space=pltpu.SMEM),
            pl.BlockSpec(memory_space=pltpu.VMEM),
            pl.BlockSpec(memory_space=pltpu.VMEM),
        ],
        out_specs=pl.BlockSpec(memory_space=pltpu.VMEM),
        cost_estimate=pl.CostEstimate(flops=8 * count * width, bytes_accessed=2 * members * count * width, transcendentals=8),
        compiler_params=room(4),
        name="spread",
        interpret=INTERPRET,
    )(repeat_index, rows, gains)


def slab_loads(chosen, sources, slabs, arrived):
    return [
        pltpu.make_async_copy(source.at[chosen], slab, arrived.at[index])
        for index, (source, slab) in enumerate(zip(sources, slabs))
    ]


def store_halves(gate_ref, up_ref, down_ref, half_refs):
    width, lanes = gate_ref.shape
    units = lanes // 2
    gate_value = gate_ref[...].astype(jnp.float32)
    up_value = up_ref[...].astype(jnp.float32)
    first = lax.broadcasted_iota(jnp.int32, (width, lanes), 1) < units
    mixed = (
        jnp.where(first, gate_value, pltpu.roll(up_value, units, 1)),
        jnp.where(first, pltpu.roll(gate_value, units, 1), up_value),
    )
    for half, half_ref in enumerate(half_refs):
        half_ref[0:width] = mixed[half].astype(half_ref.dtype)
        for column in range(width // lanes):
            start = width + column * units
            half_ref[start : start + units] = down_ref[
                half * units : (half + 1) * units, column * lanes : (column + 1) * lanes
            ]


def pack_kernel(tick, chosen_ref, gate_hbm, up_hbm, down_hbm, packed_ref, arrived):
    chosen = chosen_ref[tick]
    width, lanes = gate_hbm.shape[1:]
    moves = [
        (gate_hbm.at[chosen], packed_ref.at[0:width]),
        (up_hbm.at[chosen], packed_ref.at[width : 2 * width]),
    ]
    for column in range(width // lanes):
        start = 2 * width + column * lanes
        moves.append(
            (
                down_hbm.at[chosen, :, column * lanes : (column + 1) * lanes],
                packed_ref.at[start : start + lanes],
            )
        )
    copies = [pltpu.make_async_copy(*move, arrived.at[index]) for index, move in enumerate(moves)]
    for copy in copies:
        copy.start()
    for copy in copies:
        copy.wait()


IN_HBM = pl.BlockSpec(memory_space=pltpu.HBM)
IN_VMEM = pl.BlockSpec(memory_space=pltpu.VMEM)
IN_SMEM = pl.BlockSpec(memory_space=pltpu.SMEM)


def halves_of(weight):
    _, width, lanes = weight.shape
    half = jax.ShapeDtypeStruct((width + width // 2, lanes), weight.dtype)
    return half, half


def slabs_of(*weights):
    return [pltpu.VMEM(weight.shape[1:], weight.dtype) for weight in weights]


def pack(tick, chosen, *weights):
    size = weights[0].shape[1] * weights[0].shape[2]
    return pl.pallas_call(
        lambda *refs: pack_kernel(tick, *refs),
        out_shape=jax.ShapeDtypeStruct((3 * weights[0].shape[1], weights[0].shape[2]), weights[0].dtype),
        in_specs=[IN_SMEM, IN_HBM, IN_HBM, IN_HBM],
        out_specs=IN_VMEM,
        scratch_shapes=[pltpu.SemaphoreType.DMA((2 + weights[0].shape[1] // weights[0].shape[2],))],
        cost_estimate=pl.CostEstimate(flops=6 * size, bytes_accessed=12 * size, transcendentals=0),
        compiler_params=room(60),
        name="pack",
        interpret=INTERPRET,
    )(chosen, *weights)


def begin_kernel(
    chosen_ref, rows_hbm, gain_hbm, gate_hbm, up_hbm, down_hbm, first_ref, second_ref, copies_ref, *scratch
):
    slabs, (rows_ref, gain_ref, arrived, loaded) = scratch[:3], scratch[3:]
    early = [
        pltpu.make_async_copy(rows_hbm, rows_ref, loaded.at[0]),
        pltpu.make_async_copy(gain_hbm, gain_ref, loaded.at[1]),
    ]
    for load in early:
        load.start()
    loads = slab_loads(chosen_ref[0], (gate_hbm, up_hbm, down_hbm), slabs, arrived)
    for load in loads:
        load.start()
    for load in early:
        load.wait()
    spread_kernel(0, chosen_ref, rows_ref, gain_ref, copies_ref)
    for load in loads:
        load.wait()
    store_halves(*slabs, (first_ref, second_ref))


def begin(chosen, rows, gains, weights, members):
    size = weights[0].shape[1] * weights[0].shape[2]
    return pl.pallas_call(
        begin_kernel,
        out_shape=(*halves_of(weights[0]), jax.ShapeDtypeStruct((members, *rows.shape), rows.dtype)),
        in_specs=[IN_SMEM] + [IN_HBM] * 5,
        out_specs=(IN_VMEM,) * 3,
        scratch_shapes=slabs_of(*weights)
        + [
            pltpu.VMEM(rows.shape, rows.dtype),
            pltpu.VMEM(gains.shape, gains.dtype),
            pltpu.SemaphoreType.DMA((3,)),
            pltpu.SemaphoreType.DMA((2,)),
        ],
        cost_estimate=pl.CostEstimate(flops=6 * size, bytes_accessed=12 * size, transcendentals=8),
        compiler_params=room(60),
        name="begin",
        interpret=INTERPRET,
    )(chosen, rows, gains, *weights)


def feed_forward_kernel(pieces, tokens_ref, *refs):
    own, refs = refs[:pieces], refs[pieces:]
    count = (len(refs) - 2) // 2
    sources, out_ref, held, arrived = refs[:count], refs[count], refs[count + 1 : -1], refs[-1]
    members, rows, width = tokens_ref.shape
    lanes = own[0].shape[1]
    units = lanes // pieces
    above = 2 * width // pieces
    parts = ((0, above), (above, own[0].shape[0]))
    copies = [
        [
            pltpu.make_async_copy(source.at[start:end], slot.at[start:end], arrived.at[part, index])
            for index, (source, slot) in enumerate(zip(sources, held))
        ]
        for part, (start, end) in enumerate(parts)
    ]
    for part in copies:
        for copy in part:
            copy.start()
    tokens = tokens_ref[...].reshape(members * rows, width)
    everything = (*own, *held)
    first = lax.broadcasted_iota(jnp.int32, (members * rows, lanes), 1) < units
    hidden = []
    for index in range(0, len(everything), pieces):
        shard = everything[index : index + pieces]
        if index:
            for copy in copies[0][index - pieces : index]:
                copy.wait()
        sides = (shard[0][0:width], shard[-1][above - width : above])
        value = jnp.dot(tokens, jnp.concatenate(sides, axis=1), preferred_element_type=jnp.float32)
        gate_value, up_value = value[:, :lanes], value[:, lanes:]
        if pieces == 2:
            left, right = gate_value, up_value
            gate_value = jnp.where(first, left, pltpu.roll(right, units, 1))
            up_value = jnp.where(first, pltpu.roll(left, units, 1), right)
        hidden.append((gate_value / (1.0 + jnp.exp(-gate_value)) * up_value).astype(tokens.dtype))
    hidden = jnp.concatenate(hidden, axis=1)
    for copy in copies[1]:
        copy.wait()
    for column in range(0, width // lanes, 2):
        slabs = []
        for step in range(2):
            start = above + (column + step) * units
            slabs.append(jnp.concatenate([piece[start : start + units] for piece in everything], axis=0))
        value = jnp.dot(hidden, jnp.concatenate(slabs, axis=1), preferred_element_type=jnp.float32)
        out_ref[:, :, column * lanes : (column + 2) * lanes] = value.astype(out_ref.dtype).reshape(
            members, rows, 2 * lanes
        )


def feed_forward(tokens, own, others):
    members, rows, width = tokens.shape
    pieces = len(own)
    weights = sum(piece.size for piece in (*own, *others))
    return pl.pallas_call(
        lambda *refs: feed_forward_kernel(pieces, *refs),
        out_shape=jax.ShapeDtypeStruct(tokens.shape, tokens.dtype),
        in_specs=[IN_VMEM] * (1 + pieces) + [IN_HBM] * len(others),
        out_specs=IN_VMEM,
        scratch_shapes=[pltpu.VMEM(other.shape, other.dtype) for other in others]
        + [pltpu.SemaphoreType.DMA((2, len(others)))],
        cost_estimate=pl.CostEstimate(
            flops=2 * members * rows * weights,
            bytes_accessed=2 * weights,
            transcendentals=members * rows * weights // (3 * width),
        ),
        compiler_params=room(8),
        name="ffn",
        interpret=INTERPRET,
    )(tokens, *own, *others)


def advance_kernel(parts_ref, rows_ref, out_ref):
    total = rows_ref[...].astype(jnp.float32)
    output = parts_ref[0].astype(jnp.float32)
    for member in range(1, parts_ref.shape[0]):
        output = output + parts_ref[member].astype(jnp.float32)
    out_ref[...] = (total + output).astype(out_ref.dtype)


def advance(parts, rows):
    return pl.pallas_call(
        advance_kernel,
        out_shape=jax.ShapeDtypeStruct(rows.shape, rows.dtype),
        in_specs=[pl.BlockSpec(memory_space=pltpu.VMEM)] * 2,
        out_specs=pl.BlockSpec(memory_space=pltpu.VMEM),
        cost_estimate=pl.CostEstimate(flops=parts.size, bytes_accessed=2 * parts.size, transcendentals=0),
        compiler_params=room(4),
        name="advance",
        interpret=INTERPRET,
    )(parts, rows)


def on_device(buffer, gate_weight, up_weight, down_weight, norm_gain, repeat_index):
    current = buffer[0]
    chosen = repeat_index.reshape(TICKS)
    weights = (gate_weight[0], up_weight[0], down_weight[0])
    groups = same_kind("dp")
    members = len(groups[0])
    for tick in range(TICKS):
        if tick == 0:
            *own, copies = begin(chosen, current, norm_gain[0], weights, members)
        else:
            own = [pack(tick, chosen, *weights)]
            copies = spread(tick, chosen, current, norm_gain[0], members)
        near, pair, far = [], [], []
        for index, packed in enumerate(own):
            near.append(to_other_colour(packed, "dp", 1 if tick or index else -1))
            pair.append(to_other_core(packed, "dp"))
            far.append(to_other_core(near[-1], "dp"))
        tokens = exchange(copies, "dp", groups)
        partial_value = feed_forward(tokens, own, (*pair, *near, *far))
        parts = exchange(partial_value, "dp", groups)
        advanced = advance(parts, current)
        current = passed_along(advanced, "section", 1)
    return current[None]


def solution(mesh):
    placed = (
        P("section", "dp", None),
        P("section", None, None, "dp"),
        P("section", None, None, "dp"),
        P("section", None, "dp", None),
        P("section", None, None),
        P(None, "section"),
    )
    return jax.shard_map(
        on_device, mesh=mesh, in_specs=placed, out_specs=P("section", "dp", None), check_vma=False
    )
```

```python
import jax
import jax.numpy as jnp
from jax import lax
from jax.experimental import pallas as pl
from jax.experimental.pallas import tpu as pltpu
from jax.sharding import PartitionSpec as P


TICKS = 2
INTERPRET = False


epsilon = 0.5


def passed_along(block, axis, distance):
    devices = range(lax.axis_size(axis))
    route = [((i - distance) % len(devices), i) for i in devices]
    return lax.ppermute(block, axis, route)


def colour(place):
    return (place >> 1 ^ place >> 3) & 1


def same_kind(axis):
    places = sorted(range(lax.axis_size(axis)), key=lambda place: (place & 7, place))
    return [
        [place for place in places if place & 1 == core and colour(place) == shade]
        for core in range(2)
        for shade in range(2)
    ]


def to_other_core(value, axis):
    return lax.ppermute(value, axis, [(place, place ^ 1) for place in range(lax.axis_size(axis))])


def to_other_colour(value, axis, step):
    size = lax.axis_size(axis)
    route = [(place, place ^ 2 if place & 1 else (place + 8 * step) % size) for place in range(size)]
    return lax.ppermute(value, axis, route)


def exchange(blocks, axis, groups):
    return lax.all_to_all(blocks, axis, 0, 0, tiled=True, axis_index_groups=groups)


def room(mebibytes):
    return pltpu.CompilerParams(vmem_limit_bytes=mebibytes << 20)


def spread_kernel(tick, chosen_ref, rows_ref, gain_ref, copies_ref):
    widened = rows_ref[...].astype(jnp.float32)
    squares = jnp.mean(widened * widened, axis=-1, keepdims=True)
    gain_row = gain_ref[pl.ds(chosen_ref[tick], 1), :]
    normed = (widened * lax.rsqrt(squares + epsilon) * gain_row).astype(copies_ref.dtype)
    for member in range(copies_ref.shape[0]):
        copies_ref[member] = normed


def spread(tick, repeat_index, rows, gains, members):
    count, width = rows.shape
    return pl.pallas_call(
        lambda *refs: spread_kernel(tick, *refs),
        out_shape=jax.ShapeDtypeStruct((members, count, width), rows.dtype),
        in_specs=[
            pl.BlockSpec(memory_space=pltpu.SMEM),
            pl.BlockSpec(memory_space=pltpu.VMEM),
            pl.BlockSpec(memory_space=pltpu.VMEM),
        ],
        out_specs=pl.BlockSpec(memory_space=pltpu.VMEM),
        cost_estimate=pl.CostEstimate(flops=8 * count * width, bytes_accessed=2 * members * count * width, transcendentals=8),
        compiler_params=room(4),
        name="spread",
        interpret=INTERPRET,
    )(repeat_index, rows, gains)


def slab_loads(chosen, sources, slabs, arrived):
    return [
        pltpu.make_async_copy(source.at[chosen], slab, arrived.at[index])
        for index, (source, slab) in enumerate(zip(sources, slabs))
    ]


def store_halves(gate_ref, up_ref, down_ref, half_refs):
    width, lanes = gate_ref.shape
    units = lanes // 2
    gate_value = gate_ref[...].astype(jnp.float32)
    up_value = up_ref[...].astype(jnp.float32)
    first = lax.broadcasted_iota(jnp.int32, (width, lanes), 1) < units
    mixed = (
        jnp.where(first, gate_value, pltpu.roll(up_value, units, 1)),
        jnp.where(first, pltpu.roll(gate_value, units, 1), up_value),
    )
    for half, half_ref in enumerate(half_refs):
        half_ref[0:width] = mixed[half].astype(half_ref.dtype)
        for column in range(width // lanes):
            start = width + column * units
            half_ref[start : start + units] = down_ref[
                half * units : (half + 1) * units, column * lanes : (column + 1) * lanes
            ]


def pack_kernel(tick, chosen_ref, gate_hbm, up_hbm, down_hbm, packed_ref, arrived):
    chosen = chosen_ref[tick]
    width, lanes = gate_hbm.shape[1:]
    moves = [
        (gate_hbm.at[chosen], packed_ref.at[0:width]),
        (up_hbm.at[chosen], packed_ref.at[width : 2 * width]),
    ]
    for column in range(width // lanes):
        start = 2 * width + column * lanes
        moves.append(
            (
                down_hbm.at[chosen, :, column * lanes : (column + 1) * lanes],
                packed_ref.at[start : start + lanes],
            )
        )
    copies = [pltpu.make_async_copy(*move, arrived.at[index]) for index, move in enumerate(moves)]
    for copy in copies:
        copy.start()
    for copy in copies:
        copy.wait()


IN_HBM = pl.BlockSpec(memory_space=pltpu.HBM)
IN_VMEM = pl.BlockSpec(memory_space=pltpu.VMEM)
IN_SMEM = pl.BlockSpec(memory_space=pltpu.SMEM)


def halves_of(weight):
    _, width, lanes = weight.shape
    half = jax.ShapeDtypeStruct((width + width // 2, lanes), weight.dtype)
    return half, half


def slabs_of(*weights):
    return [pltpu.VMEM(weight.shape[1:], weight.dtype) for weight in weights]


def pack(tick, chosen, *weights):
    size = weights[0].shape[1] * weights[0].shape[2]
    return pl.pallas_call(
        lambda *refs: pack_kernel(tick, *refs),
        out_shape=jax.ShapeDtypeStruct((3 * weights[0].shape[1], weights[0].shape[2]), weights[0].dtype),
        in_specs=[IN_SMEM, IN_HBM, IN_HBM, IN_HBM],
        out_specs=IN_VMEM,
        scratch_shapes=[pltpu.SemaphoreType.DMA((2 + weights[0].shape[1] // weights[0].shape[2],))],
        cost_estimate=pl.CostEstimate(flops=6 * size, bytes_accessed=12 * size, transcendentals=0),
        compiler_params=room(60),
        name="pack",
        interpret=INTERPRET,
    )(chosen, *weights)


def begin_kernel(
    chosen_ref, rows_hbm, gain_hbm, gate_hbm, up_hbm, down_hbm, first_ref, second_ref, copies_ref, *scratch
):
    slabs, (rows_ref, gain_ref, arrived, loaded) = scratch[:3], scratch[3:]
    early = [
        pltpu.make_async_copy(rows_hbm, rows_ref, loaded.at[0]),
        pltpu.make_async_copy(gain_hbm, gain_ref, loaded.at[1]),
    ]
    for load in early:
        load.start()
    loads = slab_loads(chosen_ref[0], (gate_hbm, up_hbm, down_hbm), slabs, arrived)
    for load in loads:
        load.start()
    for load in early:
        load.wait()
    spread_kernel(0, chosen_ref, rows_ref, gain_ref, copies_ref)
    for load in loads:
        load.wait()
    store_halves(*slabs, (first_ref, second_ref))


def begin(chosen, rows, gains, weights, members):
    size = weights[0].shape[1] * weights[0].shape[2]
    return pl.pallas_call(
        begin_kernel,
        out_shape=(*halves_of(weights[0]), jax.ShapeDtypeStruct((members, *rows.shape), rows.dtype)),
        in_specs=[IN_SMEM] + [IN_HBM] * 5,
        out_specs=(IN_VMEM,) * 3,
        scratch_shapes=slabs_of(*weights)
        + [
            pltpu.VMEM(rows.shape, rows.dtype),
            pltpu.VMEM(gains.shape, gains.dtype),
            pltpu.SemaphoreType.DMA((3,)),
            pltpu.SemaphoreType.DMA((2,)),
        ],
        cost_estimate=pl.CostEstimate(flops=6 * size, bytes_accessed=12 * size, transcendentals=8),
        compiler_params=room(60),
        name="begin",
        interpret=INTERPRET,
    )(chosen, rows, gains, *weights)


def feed_forward_kernel(pieces, near_by, tokens_ref, *refs):
    resident, refs = refs[:near_by], refs[near_by:]
    count = (len(refs) - 1) // 2
    sources, out_ref, held, arrived = refs[:count], refs[count], refs[count + 1 : 2 * count + 1], refs[-1]
    members, rows, width = tokens_ref.shape
    lanes = resident[0].shape[1]
    units = lanes // pieces
    above = 2 * width // pieces
    size = 3 * width // pieces
    own = [ref.at[start : start + size] for ref in resident for start in range(0, ref.shape[0], size)]
    parts = ((0, above), (above, size))
    copies = [
        [
            pltpu.make_async_copy(source.at[start:end], slot.at[start:end], arrived.at[part, index])
            for index, (source, slot) in enumerate(zip(sources, held))
        ]
        for part, (start, end) in enumerate(parts)
    ]
    for part in copies:
        for copy in part:
            copy.start()
    tokens = tokens_ref[...].reshape(members * rows, width)
    everything = (*own, *held)
    first = lax.broadcasted_iota(jnp.int32, (members * rows, lanes), 1) < units
    hidden = []
    for index in range(0, len(everything), pieces):
        shard = everything[index : index + pieces]
        if index >= len(own):
            for copy in copies[0][index - len(own) : index - len(own) + pieces]:
                copy.wait()
        sides = (shard[0][0:width], shard[-1][above - width : above])
        value = jnp.dot(tokens, jnp.concatenate(sides, axis=1), preferred_element_type=jnp.float32)
        gate_value, up_value = value[:, :lanes], value[:, lanes:]
        if pieces == 2:
            left, right = gate_value, up_value
            gate_value = jnp.where(first, left, pltpu.roll(right, units, 1))
            up_value = jnp.where(first, pltpu.roll(left, units, 1), right)
        hidden.append((gate_value / (1.0 + jnp.exp(-gate_value)) * up_value).astype(tokens.dtype))
    hidden = jnp.concatenate(hidden, axis=1)
    for copy in copies[1]:
        copy.wait()
    for column in range(0, width // lanes, 2):
        slabs = []
        for step in range(2):
            start = above + (column + step) * units
            slabs.append(jnp.concatenate([piece[start : start + units] for piece in everything], axis=0))
        value = jnp.dot(hidden, jnp.concatenate(slabs, axis=1), preferred_element_type=jnp.float32)
        out_ref[:, :, column * lanes : (column + 2) * lanes] = value.astype(out_ref.dtype).reshape(
            members, rows, 2 * lanes
        )


def feed_forward(tokens, pieces, resident, others):
    members, rows, width = tokens.shape
    weights = sum(piece.size for piece in (*resident, *others))
    arrived = [pltpu.SemaphoreType.DMA((2, len(others)))] if others else []
    return pl.pallas_call(
        lambda *refs: feed_forward_kernel(pieces, len(resident), *refs),
        out_shape=jax.ShapeDtypeStruct(tokens.shape, tokens.dtype),
        in_specs=[IN_VMEM] * (1 + len(resident)) + [IN_HBM] * len(others),
        out_specs=IN_VMEM,
        scratch_shapes=[pltpu.VMEM(other.shape, other.dtype) for other in others] + arrived,
        cost_estimate=pl.CostEstimate(
            flops=2 * members * rows * weights,
            bytes_accessed=2 * weights,
            transcendentals=members * rows * weights // (3 * width),
        ),
        compiler_params=room(8),
        name="ffn",
        interpret=INTERPRET,
    )(tokens, *resident, *others)


def advance_kernel(parts_ref, rows_ref, out_ref):
    total = rows_ref[...].astype(jnp.float32)
    output = parts_ref[0].astype(jnp.float32)
    for member in range(1, parts_ref.shape[0]):
        output = output + parts_ref[member].astype(jnp.float32)
    out_ref[...] = (total + output).astype(out_ref.dtype)


def advance(parts, rows):
    return pl.pallas_call(
        advance_kernel,
        out_shape=jax.ShapeDtypeStruct(rows.shape, rows.dtype),
        in_specs=[pl.BlockSpec(memory_space=pltpu.VMEM)] * 2,
        out_specs=pl.BlockSpec(memory_space=pltpu.VMEM),
        cost_estimate=pl.CostEstimate(flops=parts.size, bytes_accessed=2 * parts.size, transcendentals=0),
        compiler_params=room(4),
        name="advance",
        interpret=INTERPRET,
    )(parts, rows)


def on_device(buffer, gate_weight, up_weight, down_weight, norm_gain, repeat_index):
    current = buffer[0]
    chosen = repeat_index.reshape(TICKS)
    weights = (gate_weight[0], up_weight[0], down_weight[0])
    groups = same_kind("dp")
    members = len(groups[0])
    for tick in range(TICKS):
        if tick == 0:
            *own, copies = begin(chosen, current, norm_gain[0], weights, members)
        else:
            own = [pack(tick, chosen, *weights)]
            copies = spread(tick, chosen, current, norm_gain[0], members)
        near, pair, far = [], [], []
        for index, packed in enumerate(own):
            near.append(to_other_colour(packed, "dp", 1 if tick or index else -1))
            pair.append(to_other_core(packed, "dp"))
            far.append(to_other_core(near[-1], "dp"))
        tokens = exchange(copies, "dp", groups)
        others = (*pair, *near, *far)
        resident, streamed = ((*own, *others), ()) if tick else (own, others)
        partial_value = feed_forward(tokens, len(own), resident, streamed)
        parts = exchange(partial_value, "dp", groups)
        advanced = advance(parts, current)
        current = passed_along(advanced, "section", 1)
    return current[None]


def solution(mesh):
    placed = (
        P("section", "dp", None),
        P("section", None, None, "dp"),
        P("section", None, None, "dp"),
        P("section", None, "dp", None),
        P("section", None, None),
        P(None, "section"),
    )
    return jax.shard_map(
        on_device, mesh=mesh, in_specs=placed, out_specs=P("section", "dp", None), check_vma=False
    )
```
